512 devices in a mesh: dp: 8 (over y, x_lo), seq: 64 (over x_hi, z, core).
Axes of the slice: x: 4 (x_hi: 2, x_lo: 2; x = x_hi * 2 + x_lo), y: 4, z: 16, core: 2. Of those that a mesh axis runs over, the one named last changes fastest.
Arguments:
- hidden_in: bfloat16 [8, 4096, 2048], P('dp', 'seq'), may hold values from -6 to 6
- attn_gain: float32 [2048], replicated, may hold values from 0.1 to 1.9
- w_query: bfloat16 [2048, 1280], P('dp'), may hold values from -2 to 2
- w_keyval: bfloat16 [2048, 512], P('dp'), may hold values from -1 to 1
- w_output: bfloat16 [1280, 2048], P(None, 'dp'), may hold values from -0.15625 to 0.15625
- post_gain: float32 [2048], replicated, may hold values from 0.1 to 1.9
Outputs:
- hidden_out: bfloat16 [8, 4096, 2048], P('dp', 'seq')
The draws below stay inside these ranges and needn't reach their ends.
All inputs are finite; a program needn't handle non-finite values.
Results may differ from the reference program's by a relative error of at most 0.009.
Values may be sent and summed in bfloat16 or wider, within the bound.
A program may use at most 64 MiB of HBM per device.

```python
import jax
import jax.numpy as jnp
from jax import lax

D = 2048
HEADS = 5
HD = 256
EPISODES = 8
SEQLEN = 4096


def key_columns(key):
    return jax.random.truncated_normal(jax.random.fold_in(key, 11), -4.0, 4.0, (D, HD), jnp.float32) / jnp.sqrt(jnp.float32(D))


def draw_w_keyval(key, part):
    values = jax.random.truncated_normal(jax.random.fold_in(key, 12), -4.0, 4.0, (D, HD), jnp.float32) / jnp.sqrt(jnp.float32(D))
    return jnp.concatenate([key_columns(key), values], axis=1).astype(jnp.bfloat16)


def draw_w_query(key, part):
    noise = jax.random.truncated_normal(jax.random.fold_in(key, 13), -4.0, 4.0, (D, HEADS, HD), jnp.float32) / jnp.sqrt(jnp.float32(D))
    result = noise
    return result.reshape(D, HEADS * HD).astype(jnp.bfloat16)


def block_scale(own_key, dims, split, least, high):
    def one(axis_at, blocks):
        draws = jax.random.uniform(jax.random.fold_in(jax.random.fold_in(own_key, 6), axis_at), (blocks,), jnp.float32, least / len(split), high / len(split))
        return jnp.repeat(jnp.exp(draws), dims[axis_at] // blocks).reshape((-1,) + (1,) * (len(dims) - axis_at - 1))

    factor_of = one(*split[0])
    for cut in split[1:]:
        factor_of = factor_of * one(*cut)
    return factor_of


def bell_draw(stream_key, dims, scale, bound, shards=(), kind=jnp.bfloat16):
    values = scale * jax.random.normal(stream_key, dims, jnp.float32)
    if shards:
        values = values * block_scale(stream_key, dims, shards, -0.22, 0.18)
    return jnp.clip(values, -bound, bound).astype(kind)


def setup_inputs(seed: int = 0) -> dict:
    key_of = jax.random.split(jax.random.key(seed), 7)
    hidden_in = bell_draw(key_of[0], (EPISODES, SEQLEN, D), 1.0, 6.0, ((0, 8), (1, 64)))
    attn_gain = jnp.clip(1.0 + 0.18 * jax.random.normal(key_of[1], (D,), jnp.float32), 0.1, 1.9)
    w_query = draw_w_query(jax.random.fold_in(key_of[6], 71), 0)
    w_keyval = draw_w_keyval(jax.random.fold_in(key_of[6], 71), 0)
    w_output = bell_draw(key_of[4], (HEADS * HD, D), (HEADS * HD) ** -0.5, 0.15625, ((1, 8),))
    post_gain = jnp.clip(1.0 + 0.18 * jax.random.normal(key_of[5], (D,), jnp.float32), 0.1, 1.9)
    return dict(hidden_in=hidden_in, attn_gain=attn_gain, w_query=w_query, w_keyval=w_keyval, w_output=w_output, post_gain=post_gain)


def rms_norm(v, gain):
    v = v.astype(jnp.float32)
    return v * lax.rsqrt(lax.optimization_barrier(jnp.mean(v * v, axis=-1, keepdims=True)) + 1e-06) * gain

def rotary(t, positions):
    half = t.shape[-1] // 2
    freq = jnp.exp(-jnp.log(10000.0) * jnp.arange(half, dtype=jnp.float32) * 2.0 / t.shape[-1])
    angle = positions.astype(jnp.float32)[:, None, None] * freq[None, None, :]
    cosine = jnp.cos(angle)
    sine = jnp.sin(angle)
    first = t[..., :half]
    second = t[..., half:]
    return jnp.concatenate([first * cosine - second * sine, second * cosine + first * sine], axis=-1)

def reference(hidden_in, attn_gain, w_query, w_keyval, w_output, post_gain):

    def episode(frame):
        normed = rms_norm(frame, attn_gain).astype(jnp.bfloat16)
        query_raw = jnp.dot(normed, w_query, preferred_element_type=jnp.float32)
        keyval_raw = jnp.dot(normed, w_keyval, preferred_element_type=jnp.float32)
        positions = jnp.arange(SEQLEN, dtype=jnp.int32)
        query = (rotary(query_raw.reshape(SEQLEN, HEADS, HD), positions) * HD ** (-0.5)).astype(jnp.bfloat16)
        keys = rotary(keyval_raw[:, None, :HD], positions)[:, 0, :].astype(jnp.bfloat16)
        values = keyval_raw[:, HD:].astype(jnp.bfloat16)

        def one_head(query_head):
            scores = jnp.dot(query_head, keys.T, preferred_element_type=jnp.float32)
            rowmax = lax.optimization_barrier(jnp.max(scores, axis=1, keepdims=True))
            expo = jnp.exp(scores - rowmax)
            total = lax.optimization_barrier(jnp.sum(expo, axis=1, keepdims=True))
            summed = jnp.dot(expo.astype(jnp.bfloat16), values, preferred_element_type=jnp.float32)
            return summed / total
        heads = lax.map(one_head, jnp.transpose(query, (1, 0, 2)))
        attended = jnp.transpose(heads, (1, 0, 2)).reshape(SEQLEN, HEADS * HD).astype(jnp.bfloat16)
        projected = jnp.dot(attended, w_output, preferred_element_type=jnp.float32)
        return (frame.astype(jnp.float32) + rms_norm(projected, post_gain)).astype(jnp.bfloat16)
    return lax.map(episode, hidden_in)
```

```python
import functools

import jax
import jax.numpy as jnp
from jax import lax
from jax.experimental import pallas as pl
from jax.experimental.pallas import tpu as pltpu
from jax.sharding import PartitionSpec as P

BF16 = jnp.bfloat16
F32 = jnp.float32

ROWS = 64
HD = 256
HEADS = 5
NCH = 2 + HEADS + HEADS
NZ = 16
HALF = NZ // 2


def ring_kernel(
    hid, gain, cos, sin, pgain, wq, wkv, wo, out,
    wbuf, kvbuf, nrel, qbuf, acc, mrow, lrow, proj,
    lsem, wss, wrs, kss, krs, css, crs,
):
    dp = lax.axis_index("dp")
    sq = lax.axis_index("seq")
    y, xl = dp // 2, dp % 2
    xh, z, c = sq // 32, (sq // 2) % NZ, sq % 2

    def dev(yy, xll, xhh, zz, cc):
        return (yy * 2 + xll, xhh * 32 + zz * 2 + cc)

    yp = dev((y + 1) % 4, xl, xh, z, c)
    ym = dev((y + 3) % 4, xl, xh, z, c)
    xp = dev(y, 1 - xl, (xh + xl) % 2, z, c)
    xm = dev(y, 1 - xl, (xh + 1 - xl) % 2, z, c)
    xo = dev(y, xl, 1 - xh, z, c)
    zp = dev(y, xl, xh, (z + 1) % NZ, c)
    zm = dev(y, xl, xh, (z + NZ - 1) % NZ, c)
    co = dev(y, xl, xh, z, 1 - c)

    def load(ch):
        if ch < 2:
            src = wkv.at[:, pl.ds(ch * HD, HD)]
        elif ch < 2 + HEADS:
            src = wq.at[:, pl.ds((ch - 2) * HD, HD)]
        else:
            src = wo.at[pl.ds((ch - 2 - HEADS) * HD, HD), :]
        return pltpu.make_async_copy(src, wbuf.at[ch, 0], lsem.at[ch])

    for ch in range(NCH):
        load(ch).start()

    barrier = pltpu.get_barrier_semaphore()
    for peer in (yp, ym, xp, xm, xo, zp, zm, co):
        pl.semaphore_signal(
            barrier, inc=1, device_id=peer, device_id_type=pl.DeviceIdType.MESH
        )
    pl.semaphore_wait(barrier, 8)

    def mine(n, h=0):
        return pl.ds(pl.multiple_of(c * 128 + h * 64, 64), n)

    def wcopy(ch, k, src_slots, dst_slots, rows, peer):
        return pltpu.make_async_remote_copy(
            src_ref=wbuf.at[ch, src_slots, rows],
            dst_ref=wbuf.at[ch, dst_slots, rows],
            send_sem=wss.at[ch, k],
            recv_sem=wrs.at[ch, k],
            device_id=peer,
            device_id_type=pl.DeviceIdType.MESH,
        )

    def y_own(ch):
        return [
            wcopy(ch, 0, 0, 1, mine(128), yp),
            wcopy(ch, 1, 0, 2, mine(128), ym),
        ]

    def y_relay(ch):
        return [
            wcopy(ch, 2, 1, 3, mine(64, 0), yp),
            wcopy(ch, 3, 2, 3, mine(64, 1), ym),
        ]

    def x_own(ch):
        return [
            wcopy(ch, 4, 0, 4, mine(64, 0), xp),
            wcopy(ch, 5, 0, 4, mine(64, 1), xm),
        ]

    def x_near(ch):
        near, far = pl.ds(1, 2), pl.ds(5, 2)
        return [
            wcopy(ch, 6, near, far, mine(64, 0), xp),
            wcopy(ch, 7, near, far, mine(64, 1), xm),
        ]

    def x_far(ch):
        return [
            wcopy(ch, 8, 3, 7, mine(64, 0), xp),
            wcopy(ch, 9, 3, 7, mine(64, 1), xm),
        ]

    def c_near(ch):
        return [wcopy(ch, 10, pl.ds(1, 2), pl.ds(1, 2), mine(128), co)]

    def c_far(ch):
        return [wcopy(ch, 11, 3, 3, mine(128), co)]

    def c_side(ch):
        return [wcopy(ch, 12, pl.ds(4, 4), pl.ds(4, 4), mine(128), co)]

    def start(copies):
        for d in copies:
            d.start()

    def arrived(copies):
        for d in copies:
            d.wait_recv()

    def sent(copies):
        for d in copies:
            d.wait_send()

    def step0(ch):
        start(y_own(ch) + x_own(ch))

    def step1(ch):
        arrived(y_own(ch))
        start(y_relay(ch) + x_near(ch) + c_near(ch))

    def step2(ch):
        arrived(y_relay(ch))
        start(x_far(ch) + c_far(ch))

    def step3(ch):
        arrived(x_own(ch) + x_near(ch) + x_far(ch))
        start(c_side(ch))

    def whole(ch):
        arrived(c_near(ch) + c_far(ch) + c_side(ch))

    def kvcopy(k, src, dst, peer):
        g, j, n = dst
        return pltpu.make_async_remote_copy(
            src_ref=kvbuf.at[src[0], 0, pl.ds(src[1], n)],
            dst_ref=kvbuf.at[g, 0, pl.ds(j, n)],
            send_sem=kss.at[g, k],
            recv_sem=krs.at[g, k],
            device_id=peer,
            device_id_type=pl.DeviceIdType.MESH,
        )

    xhi = kvcopy(0, (0, 0), (0, 1, 1), xo)

    def ring(s, j):
        first = isinstance(s, int) and s == 1
        src = (0, j % 2) if first else (s - 1, j)
        return kvcopy(j, src, (s, j, 1), zp if j < 2 else zm)

    last = [
        kvcopy(2, (HALF - 1, 0), (0, 2, 1), zp),
        kvcopy(3, (HALF - 1, 3), (0, 3, 1), zm),
    ]

    def cross(g, j, n, k):
        return pltpu.make_async_remote_copy(
            src_ref=kvbuf.at[g, 0, pl.ds(j, n)],
            dst_ref=kvbuf.at[g, 1, pl.ds(j, n)],
            send_sem=css.at[g, k],
            recv_sem=crs.at[g, k],
            device_id=co,
            device_id_type=pl.DeviceIdType.MESH,
        )

    cross_own = cross(0, 0, 1, 0)
    cross_xhi = cross(0, 1, 1, 1)
    cross_far = cross(0, 2, 2, 2)

    def norm(v, eps=1e-06):
        return lax.rsqrt(jnp.mean(v * v, axis=-1, keepdims=True) + eps)

    def column(slot):
        yy = (y + (0, 3, 1, 2)[slot % 4]) % 4
        xx = xl if slot < 4 else 1 - xl
        return pl.ds(pl.multiple_of((yy * 2 + xx) * HD, HD), HD)

    def projected(ch):
        w = wbuf[ch].reshape(8 * HD, HD)
        return jnp.dot(nrel[...], w, preferred_element_type=F32)

    def rotary(u):
        first, second = u[:, : HD // 2], u[:, HD // 2 :]
        cs, sn = cos[...], sin[...]
        return jnp.concatenate(
            [first * cs - second * sn, second * cs + first * sn], axis=1
        )

    def query(ch, head):
        whole(ch)
        q = rotary(projected(ch)) * HD ** (-0.5)
        qbuf[pl.ds(head * ROWS, ROWS), :] = q.astype(BF16)

    def attend(g):
        kv = kvbuf[g].reshape(8 * ROWS, 2 * HD)
        keys, values = kv[:, :HD], kv[:, HD:]
        s = lax.dot_general(
            qbuf[...], keys, (((1,), (1,)), ((), ())), preferred_element_type=F32
        )
        old = mrow[:, :1]
        new = jnp.maximum(old, jnp.max(s, axis=1, keepdims=True))
        scale = jnp.exp(old - new)
        e = jnp.exp(s - new)
        lrow[...] = lrow[...] * scale + jnp.sum(e, axis=1, keepdims=True)
        mrow[...] = jnp.broadcast_to(new, mrow.shape)
        acc[...] = acc[...] * scale + jnp.dot(
            e.astype(BF16), values, preferred_element_type=F32
        )

    load(0).wait()
    load(1).wait()
    step0(0)
    step0(1)
    for ch in range(2, NCH):
        load(ch).wait()

    hidden = hid[...].astype(F32)
    inv = norm(hidden)
    for slot in range(8):
        col = column(slot)
        part = hid[:, col].astype(F32) * inv * gain[:, col]
        nrel[:, slot * HD : (slot + 1) * HD] = part.astype(BF16)
    acc[...] = jnp.zeros_like(acc)
    lrow[...] = jnp.zeros_like(lrow)
    mrow[...] = jnp.full_like(mrow, -1e30)

    step1(0)
    step1(1)
    step0(2)
    step2(0)
    step2(1)
    step0(3)
    step1(2)
    step3(0)
    step3(1)
    step2(2)
    step1(3)
    step0(4)

    whole(0)
    k = rotary(projected(0))
    kvbuf[0, 0, 0, :, :HD] = k.astype(BF16)
    whole(1)
    kvbuf[0, 0, 0, :, HD:] = projected(1).astype(BF16)

    xhi.start()
    ring(1, 0).start()
    ring(1, 2).start()
    cross_own.start()
    step3(2)
    step2(3)
    step1(4)
    step0(5)
    xhi.wait_recv()
    ring(1, 1).start()
    ring(1, 3).start()
    cross_xhi.start()

    def turn(s):
        for j in range(4):
            ring(s - 1, j).wait_recv()
            ring(s, j).start()
        cross(s - 1, 0, 4, 0).start()

    def weights(i):
        step3(i - 2)
        step2(i - 1)
        step1(i)
        step0(i + 1)

    def early(s, _):
        for j in range(4):
            kvcopy(j, (s - 1, j), (s - 1, j, 1), zp).wait_recv()
            ring(s, j).start()
        cross(s - 1, 0, 4, 0).start()
        weights(s + 3)
        query(s, s - 2)
        return 0

    lax.fori_loop(2, 6, early, 0)

    def groups(a, b):
        def one(g, _):
            cross(g, 0, 4, 0).wait_recv()
            attend(g)
            return 0

        lax.fori_loop(a, b, one, 0)

    turn(6)
    weights(9)
    query(6, 4)
    groups(1, 3)
    turn(7)
    weights(10)
    groups(3, 5)
    for j in range(4):
        ring(HALF - 1, j).wait_recv()
    for d in last:
        d.start()
    cross(HALF - 1, 0, 4, 0).start()
    step3(9)
    step2(10)
    step1(11)
    groups(5, 7)
    for d in last:
        d.wait_recv()
    cross_far.start()
    step3(10)
    step2(11)
    groups(7, 8)
    cross_own.wait_recv()
    cross_xhi.wait_recv()
    cross_far.wait_recv()
    step3(11)
    attend(0)

    att = (acc[...] / lrow[:, :1]).astype(BF16)
    for ch in range(2 + HEADS, NCH):
        whole(ch)
    total = jnp.zeros((ROWS, 1), F32)
    for slot in range(8):
        part = jnp.zeros((ROWS, HD), F32)
        for h in range(HEADS):
            part += jnp.dot(
                att[h * ROWS : (h + 1) * ROWS],
                wbuf[2 + HEADS + h, slot],
                preferred_element_type=F32,
            )
        proj[:, slot * HD : (slot + 1) * HD] = part
        total += jnp.sum(part * part, axis=1, keepdims=True)
    inv2 = lax.rsqrt(total / (8 * HD) + 1e-06)
    for slot in range(8):
        col = column(slot)
        part = proj[:, slot * HD : (slot + 1) * HD] * inv2 * pgain[:, col]
        out[:, col] = (hid[:, col].astype(F32) + part).astype(BF16)

    def drain(ch, _):
        sent(
            y_own(ch) + y_relay(ch) + x_own(ch) + x_near(ch) + x_far(ch)
            + c_near(ch) + c_far(ch) + c_side(ch)
        )
        return 0

    lax.fori_loop(0, NCH, drain, 0)

    def drain_ring(g, _):
        for j in range(4):
            kvcopy(j, (g, j), (g, j, 1), zp).wait_send()
        cross(g, 0, 4, 0).wait_send()
        return 0

    lax.fori_loop(1, HALF, drain_ring, 0)
    sent([xhi, cross_own, cross_xhi, cross_far] + last)


def local(hidden_in, attn_gain, w_query, w_keyval, w_output, post_gain):
    count, width = hidden_in.shape[1:]
    freq = jnp.exp(-jnp.log(10000.0) * jnp.arange(HD // 2, dtype=F32) * 2.0 / HD)
    positions = lax.axis_index("seq") * count + jnp.arange(count, dtype=jnp.int32)
    angle = positions.astype(F32)[:, None] * freq[None, :]
    vmem = pl.BlockSpec(memory_space=pltpu.VMEM)
    hbm = pl.BlockSpec(memory_space=pl.ANY)
    dma = pltpu.SemaphoreType.DMA
    result = pl.pallas_call(
        ring_kernel,
        out_shape=jax.ShapeDtypeStruct((count, width), BF16),
        in_specs=[vmem] * 5 + [hbm] * 3,
        out_specs=vmem,
        scratch_shapes=[
            pltpu.VMEM((NCH, 8, HD, HD), BF16),
            pltpu.VMEM((HALF, 2, 4, ROWS, 2 * HD), BF16),
            pltpu.VMEM((ROWS, 8 * HD), BF16),
            pltpu.VMEM((HEADS * ROWS, HD), BF16),
            pltpu.VMEM((HEADS * ROWS, HD), F32),
            pltpu.VMEM((HEADS * ROWS, 128), F32),
            pltpu.VMEM((HEADS * ROWS, 128), F32),
            pltpu.VMEM((ROWS, 8 * HD), F32),
            dma((NCH,)),
            dma((NCH, 13)),
            dma((NCH, 13)),
            dma((HALF, 4)),
            dma((HALF, 4)),
            dma((HALF, 3)),
            dma((HALF, 3)),
        ],
        compiler_params=pltpu.CompilerParams(
            collective_id=0, has_side_effects=True, vmem_limit_bytes=60 * 1024 * 1024
        ),
    )(
        hidden_in[0], attn_gain[None], jnp.cos(angle), jnp.sin(angle), post_gain[None],
        w_query, w_keyval, w_output,
    )
    return result[None]


def solution(mesh):
    return jax.shard_map(
        local,
        mesh=mesh,
        in_specs=(
            P("dp", "seq", None), P(), P("dp", None), P("dp", None), P(None, "dp"), P(),
        ),
        out_specs=P("dp", "seq", None),
        check_vma=False,
    )
```

```python
import jax
import jax.numpy as jnp
import numpy as np
from jax import lax
from jax.experimental import pallas as pl
from jax.experimental.pallas import tpu as pltpu
from jax.sharding import PartitionSpec as P

BF16 = jnp.bfloat16
F32 = jnp.float32

ROWS = 64
HD = 256
HEADS = 5
QS, OS = 2, 2 + HEADS
NCH = OS + HEADS
NZ = 16
HALF = NZ // 2
MESH = pl.DeviceIdType.MESH


def ring_kernel(
    hid, gain, crow, srow, cbase, sbase, pgain, wq, wkv, wo, out,
    wbuf, kvbuf, nrel, qbuf, qout, acc, mrow, lrow, proj, cos, sin,
    lsem, wss, wcs, wrs, wrc, krs, kss, xss, xrs, css, crs, nss, nrs, qss, qrs,
):
    dp = lax.axis_index("dp")
    sq = lax.axis_index("seq")
    y, xl = dp // 2, dp % 2
    xh, z, c = sq // 32, (sq // 2) % NZ, sq % 2

    def dev(yy, xll, xhh, zz, cc):
        return (yy * 2 + xll, xhh * 32 + zz * 2 + cc)

    yp = dev((y + 1) % 4, xl, xh, z, c)
    ym = dev((y + 3) % 4, xl, xh, z, c)
    xp = dev(y, 1 - xl, (xh + xl) % 2, z, c)
    xm = dev(y, 1 - xl, (xh + 1 - xl) % 2, z, c)
    xo = dev(y, xl, 1 - xh, z, c)
    zp = dev(y, xl, xh, (z + 1) % NZ, c)
    zm = dev(y, xl, xh, (z + NZ - 1) % NZ, c)
    co = dev(y, xl, xh, z, 1 - c)

    def remote(src, dst, ssem, rsem, peer):
        return pltpu.make_async_remote_copy(
            src_ref=src, dst_ref=dst, send_sem=ssem, recv_sem=rsem,
            device_id=peer, device_id_type=MESH,
        )

    def awaited(ref, sem):
        pltpu.make_async_copy(ref, ref, sem).wait()

    def load(ch):
        if ch < QS:
            src = wkv.at[:, pl.ds(ch * HD, HD)]
        elif ch < OS:
            src = wq.at[:, pl.ds((ch - QS) * HD, HD)]
        else:
            src = wo.at[pl.ds((ch - OS) * HD, HD), :]
        sem = lsem.at[0 if ch < QS else 1]
        pltpu.make_async_copy(src, wbuf.at[ch, 0], sem).start()

    @pl.when(c == 1)
    def _():
        for ch in (0, 1, *range(OS, NCH)):
            load(ch)

    @pl.when(c == 0)
    def _():
        for ch in range(QS, NCH):
            load(ch)

    barrier = pltpu.get_barrier_semaphore()
    for peer in (yp, ym, xp, xm, xo, zp, zm, co):
        pl.semaphore_signal(barrier, inc=1, device_id=peer, device_id_type=MESH)
    pl.semaphore_wait(barrier, 8)

    top, bottom, every = pl.ds(0, 128), pl.ds(128, 128), pl.ds(0, 256)

    def wcopy(ch, kind, src, dst, rows, peer):
        remote(
            wbuf.at[ch, src, rows], wbuf.at[ch, dst, rows],
            wss.at[0], wrs.at[ch, kind], peer,
        ).start()

    def step0(ch):
        wcopy(ch, 0, 0, 1, every, yp)
        wcopy(ch, 0, 0, 2, every, ym)
        wcopy(ch, 2, 0, 4, top, xp)
        wcopy(ch, 2, 0, 4, bottom, xm)

    def step1(ch):
        awaited(wbuf.at[ch, pl.ds(1, 2)], wrs.at[ch, 0])
        wcopy(ch, 1, 1, 3, top, yp)
        wcopy(ch, 1, 2, 3, bottom, ym)
        wcopy(ch, 2, pl.ds(1, 2), pl.ds(5, 2), top, xp)
        wcopy(ch, 2, pl.ds(1, 2), pl.ds(5, 2), bottom, xm)

    def step2(ch):
        awaited(wbuf.at[ch, 3], wrs.at[ch, 1])
        wcopy(ch, 2, 3, 7, top, xp)
        wcopy(ch, 2, 3, 7, bottom, xm)

    def step3(ch):
        awaited(wbuf.at[ch, pl.ds(4, 4)], wrs.at[ch, 2])

    def pass_on(ch, slots):
        ref = wbuf.at[ch, slots]
        remote(ref, ref, wcs.at[0], wrc.at[ch - OS], co).start()

    def give(ch):
        pass_on(ch, pl.ds(1, 3))
        step3(ch)
        pass_on(ch, pl.ds(4, 4))

    def hop(src, dst, half, peer):
        remote(
            kvbuf.at[src[0], src[1], half], kvbuf.at[dst[0], dst[1], half],
            kss.at[0], krs.at[dst[0], dst[1] // 2, half], peer,
        ).start()

    def hops(s, ab, half, first=False):
        for way, peer in ((0, zp), (1, zm)):
            src = (0, 2 * ab) if first else (s - 1, 2 * ab + way)
            hop(src, (s, 2 * ab + way), half, peer)

    def landed(s, ab, half):
        awaited(kvbuf.at[s, pl.ds(2 * ab, 2), half], krs.at[s, ab, half])

    def cross(g, js, k):
        ref = kvbuf.at[g, js]
        return remote(ref, ref, css.at[0], crs.at[g, k], co)

    def column(slot):
        yy = (y + (0, 3, 1, 2)[slot % 4]) % 4
        xx = xl if slot < 4 else 1 - xl
        return pl.ds(pl.multiple_of((yy * 2 + xx) * HD, HD), HD)

    def normalize():
        hidden = hid[...].astype(F32)
        inv = lax.rsqrt(jnp.mean(hidden * hidden, axis=-1, keepdims=True) + 1e-06)
        own = pl.ds(pl.multiple_of(c * ROWS, ROWS), ROWS)
        for slot in range(8):
            col = column(slot)
            part = hid[:, col].astype(F32) * inv * gain[:, col]
            nrel[own, slot * HD : (slot + 1) * HD] = part.astype(BF16)
        remote(nrel.at[own], nrel.at[own], nss.at[0], nrs.at[0], co).start()
        at = pl.ds(sq // 2, 1)
        cb, sb = cbase[at, :], sbase[at, :]
        cr, sr = crow[...], srow[...]
        cos[...] = cb * cr - sb * sr
        sin[...] = sb * cr + cb * sr
        acc[...] = jnp.zeros_like(acc)
        lrow[...] = jnp.zeros_like(lrow)
        mrow[...] = jnp.full_like(mrow, -1e30)

    def partner_rows():
        other = pl.ds(pl.multiple_of((1 - c) * ROWS, ROWS), ROWS)
        awaited(nrel.at[other], nrs.at[0])

    def projected(ch):
        w = wbuf[ch].reshape(8 * HD, HD)
        return jnp.dot(nrel[...], w, preferred_element_type=F32)

    def rotary(u):
        first, second = u[:, : HD // 2], u[:, HD // 2 :]
        cs, sn = cos[...], sin[...]
        return jnp.concatenate(
            [first * cs - second * sn, second * cs + first * sn], axis=1
        )

    def query(h):
        q = (rotary(projected(QS + h)) * HD ** (-0.5)).astype(BF16)
        qbuf[h] = q[:ROWS]
        qout[h] = q[ROWS:]
        remote(qout.at[h], qbuf.at[h], qss.at[0], qrs.at[0], co).start()

    def attend(g):
        kv = kvbuf[g].reshape(8 * ROWS, 2 * HD)
        keys, values = kv[:, :HD], kv[:, HD:]
        q = qbuf[...].reshape(HEADS * ROWS, HD)
        s = lax.dot_general(
            q, keys, (((1,), (1,)), ((), ())), preferred_element_type=F32
        )
        old = mrow[:, :1]
        new = jnp.maximum(old, jnp.max(s, axis=1, keepdims=True))
        scale = jnp.exp(old - new)
        e = jnp.exp(s - new)
        lrow[...] = lrow[...] * scale + jnp.sum(e, axis=1, keepdims=True)
        mrow[...] = jnp.broadcast_to(new, mrow.shape)
        acc[...] = acc[...] * scale + jnp.dot(
            e.astype(BF16), values, preferred_element_type=F32
        )

    def finish():
        att = (acc[...] / lrow[:, :1]).astype(BF16)
        total = jnp.zeros((ROWS, 1), F32)
        for slot in range(8):
            part = jnp.zeros((ROWS, HD), F32)
            for h in range(HEADS):
                part += jnp.dot(
                    att[h * ROWS : (h + 1) * ROWS], wbuf[OS + h, slot],
                    preferred_element_type=F32,
                )
            proj[:, slot * HD : (slot + 1) * HD] = part
            total += jnp.sum(part * part, axis=1, keepdims=True)
        inv = lax.rsqrt(total / (8 * HD) + 1e-06)
        for slot in range(8):
            col = column(slot)
            part = proj[:, slot * HD : (slot + 1) * HD] * inv * pgain[:, col]
            out[:, col] = (hid[:, col].astype(F32) + part).astype(BF16)

    @pl.when(c == 1)
    def _():
        awaited(wbuf.at[pl.ds(0, 2), 0], lsem.at[0])
        step0(0)
        step0(1)
        normalize()
        step1(0)
        step1(1)
        step2(0)
        step2(1)
        partner_rows()
        step3(0)
        k = rotary(projected(0)).astype(BF16)
        kvbuf[0, 0, :, :, :HD] = k.reshape(2, ROWS, HD)
        step3(1)
        v = projected(1).astype(BF16)
        kvbuf[0, 0, :, :, HD:] = v.reshape(2, ROWS, HD)
        for half in range(2):
            remote(
                kvbuf.at[0, 0, half], kvbuf.at[0, 2, half],
                xss.at[0], xrs.at[half], xo,
            ).start()
            hops(1, 0, half, True)
        cross(0, 0, 0).start()
        for half in range(2):
            awaited(kvbuf.at[0, 2, half], xrs.at[half])
            hops(1, 1, half, True)
        cross(0, 2, 1).start()

        def turn(s, ab):
            for half in range(2):
                landed(s - 1, ab, half)
                hops(s, ab, half)

        def early(s, _):
            turn(s, 0)
            turn(s, 1)
            cross(s - 1, pl.ds(0, 4), 0).start()
            return 0

        lax.fori_loop(2, 6, early, 0)

        turn(6, 0)
        turn(6, 1)
        cross(5, pl.ds(0, 4), 0).start()
        awaited(qbuf, qrs.at[0])
        attend(1)
        turn(7, 0)
        attend(2)
        turn(7, 1)
        cross(6, pl.ds(0, 4), 0).start()
        attend(3)
        for half in range(2):
            landed(HALF - 1, 0, half)
            hop((HALF - 1, 0), (0, 1), half, zp)
        attend(4)
        for half in range(2):
            landed(HALF - 1, 1, half)
            hop((HALF - 1, 3), (0, 3), half, zm)
        cross(HALF - 1, pl.ds(0, 4), 0).start()

        def rest(g, _):
            attend(g)
            return 0

        lax.fori_loop(5, HALF, rest, 0)
        for ab in range(2):
            for half in range(2):
                awaited(kvbuf.at[0, 2 * ab + 1, half], krs.at[0, ab, half])
            cross(0, 2 * ab + 1, 2 + ab).start()
        attend(0)
        awaited(wbuf.at[pl.ds(OS, HEADS), 0], lsem.at[1])
        for ch in range(OS, NCH):
            awaited(wbuf.at[ch, pl.ds(1, 7)], wrc.at[ch - OS])
        finish()
        awaited(wbuf.at[pl.ds(0, 2), pl.ds(0, 7)], wss.at[0])
        awaited(wbuf.at[pl.ds(0, 6), pl.ds(0, 5)], kss.at[0])
        awaited(kvbuf.at[0, 0], xss.at[0])
        awaited(kvbuf, css.at[0])

    @pl.when(c == 0)
    def _():
        normalize()
        awaited(wbuf.at[pl.ds(QS, 2 * HEADS), 0], lsem.at[1])
        step0(2)
        partner_rows()
        step0(3)
        step1(2)
        step0(4)
        step1(3)
        step2(2)
        step0(5)

        def queries(i, _):
            step1(i)
            step2(i - 1)
            step0(i + 2)
            step3(i - 2)
            query(i - QS - 2)
            return 0

        lax.fori_loop(4, 9, queries, 0)

        def near(g):
            awaited(kvbuf.at[g], crs.at[g, 0])
            attend(g)

        step1(9)
        step2(8)
        step0(11)
        give(7)
        near(1)
        step1(10)
        step2(9)
        near(2)
        give(8)
        step1(11)
        step2(10)
        near(3)
        give(9)
        step2(11)
        near(4)
        give(10)
        near(5)
        give(11)
        near(6)
        near(7)
        for j, k in ((0, 0), (2, 1), (1, 2), (3, 3)):
            awaited(kvbuf.at[0, j], crs.at[0, k])
        attend(0)
        finish()
        awaited(wbuf.at[pl.ds(QS, 2 * HEADS), pl.ds(0, 7)], wss.at[0])
        awaited(wbuf.at[pl.ds(OS, HEADS), pl.ds(1, 7)], wcs.at[0])
        awaited(qout, qss.at[0])

    own = pl.ds(pl.multiple_of(c * ROWS, ROWS), ROWS)
    awaited(nrel.at[own], nss.at[0])


def local(hidden_in, attn_gain, w_query, w_keyval, w_output, post_gain):
    count, width = hidden_in.shape[1:]
    freq = 10000.0 ** (-np.arange(HD // 2) * 2.0 / HD)
    row = np.arange(2 * ROWS)[:, None] * freq
    base = np.arange(2 * NZ)[:, None] * (2 * ROWS) * freq
    tables = [np.asarray(f(a), np.float32) for a in (row, base) for f in (np.cos, np.sin)]
    vmem = pl.BlockSpec(memory_space=pltpu.VMEM)
    hbm = pl.BlockSpec(memory_space=pltpu.HBM)
    dma = pltpu.SemaphoreType.DMA
    result = pl.pallas_call(
        ring_kernel,
        out_shape=jax.ShapeDtypeStruct((count, width), BF16),
        in_specs=[vmem] * 7 + [hbm] * 3,
        out_specs=vmem,
        scratch_shapes=[
            pltpu.VMEM((NCH, 8, HD, HD), BF16),
            pltpu.VMEM((HALF, 4, 2, ROWS, 2 * HD), BF16),
            pltpu.VMEM((2 * ROWS, 8 * HD), BF16),
            pltpu.VMEM((HEADS, ROWS, HD), BF16),
            pltpu.VMEM((HEADS, ROWS, HD), BF16),
            pltpu.VMEM((HEADS * ROWS, HD), F32),
            pltpu.VMEM((HEADS * ROWS, 128), F32),
            pltpu.VMEM((HEADS * ROWS, 128), F32),
            pltpu.VMEM((ROWS, 8 * HD), F32),
            pltpu.VMEM((2 * ROWS, HD // 2), F32),
            pltpu.VMEM((2 * ROWS, HD // 2), F32),
            dma((2,)),
            dma((1,)),
            dma((1,)),
            dma((NCH, 3)),
            dma((HEADS,)),
            dma((HALF, 2, 2)),
            dma((1,)),
            dma((1,)),
            dma((2,)),
            dma((1,)),
            dma((HALF, 4)),
            dma((1,)),
            dma((1,)),
            dma((1,)),
            dma((1,)),
        ],
        compiler_params=pltpu.CompilerParams(
            collective_id=0, has_side_effects=True, vmem_limit_bytes=60 * 1024 * 1024
        ),
    )(
        hidden_in[0], attn_gain[None], *tables, post_gain[None],
        w_query, w_keyval, w_output,
    )
    return result[None]


def solution(mesh):
    return jax.shard_map(
        local,
        mesh=mesh,
        in_specs=(
            P("dp", "seq", None), P(), P("dp", None), P("dp", None), P(None, "dp"), P(),
        ),
        out_specs=P("dp", "seq", None),
        check_vma=False,
    )
```

```python
import jax
import jax.numpy as jnp
import numpy as np
from jax import lax
from jax.experimental import pallas as pl
from jax.experimental.pallas import tpu as pltpu
from jax.sharding import PartitionSpec as P

BF16 = jnp.bfloat16
F32 = jnp.float32

ROWS = 64
HD = 256
HEADS = 5
QS, OS = 2, 2 + HEADS
NCH = OS + HEADS
NZ = 16
HALF = NZ // 2
PIECES = 4
PIECE = 2 * ROWS // PIECES
MESH = pl.DeviceIdType.MESH


def ring_kernel(
    hid_in, gain_in, crow_in, srow_in, cbase_in, sbase_in, pgain_in, wq, wkv, wo, out,
    hid, gain, crow, srow, cbase, sbase, pgain, wbuf, kvbuf, nrel, qbuf, qout, acc, mrow, lrow, proj, cos, sin,
    lsem, wss, wcs, wrs, wrc, krs, kss, xss, xrs, css, crs, nss, nrs, qss, qrs,
):
    dp = lax.axis_index("dp")
    sq = lax.axis_index("seq")
    y, xl = dp // 2, dp % 2
    xh, z, c = sq // 32, (sq // 2) % NZ, sq % 2

    def dev(yy, xll, xhh, zz, cc):
        return (yy * 2 + xll, xhh * 32 + zz * 2 + cc)

    yp = dev((y + 1) % 4, xl, xh, z, c)
    ym = dev((y + 3) % 4, xl, xh, z, c)
    xp = dev(y, 1 - xl, (xh + xl) % 2, z, c)
    xm = dev(y, 1 - xl, (xh + 1 - xl) % 2, z, c)
    xo = dev(y, xl, 1 - xh, z, c)
    zp = dev(y, xl, xh, (z + 1) % NZ, c)
    zm = dev(y, xl, xh, (z + NZ - 1) % NZ, c)
    co = dev(y, xl, xh, z, 1 - c)

    def remote(src, dst, ssem, rsem, peer):
        return pltpu.make_async_remote_copy(
            src_ref=src, dst_ref=dst, send_sem=ssem, recv_sem=rsem,
            device_id=peer, device_id_type=MESH,
        )

    def awaited(ref, sem):
        pltpu.make_async_copy(ref, ref, sem).wait()

    barrier = pltpu.get_barrier_semaphore()
    for peer in (yp, ym, xp, xm, xo, zp, zm, co):
        pl.semaphore_signal(barrier, inc=1, device_id=peer, device_id_type=MESH)

    def load(ch):
        if ch < QS:
            src = wkv.at[:, pl.ds(ch * HD, HD)]
        elif ch < OS:
            src = wq.at[:, pl.ds((ch - QS) * HD, HD)]
        else:
            src = wo.at[pl.ds((ch - OS) * HD, HD), :]
        sem = lsem.at[0 if ch < QS else 1]
        pltpu.make_async_copy(src, wbuf.at[ch, 0], sem).start()

    small = [
        pltpu.make_async_copy(src, dst, lsem.at[2 + i])
        for i, (src, dst) in enumerate(
            [
                (hid_in, hid), (gain_in, gain), (crow_in, crow), (srow_in, srow),
                (cbase_in, cbase), (sbase_in, sbase), (pgain_in, pgain),
            ]
        )
    ]

    @pl.when(c == 1)
    def _():
        for ch in (0, 1):
            load(ch)

    for copy in small:
        copy.start()

    @pl.when(c == 1)
    def _():
        for ch in range(OS, NCH):
            load(ch)

    @pl.when(c == 0)
    def _():
        for ch in range(QS, NCH):
            load(ch)

    pl.semaphore_wait(barrier, 8)

    top, bottom, every = pl.ds(0, 128), pl.ds(128, 128), pl.ds(0, 256)

    def wcopy(ch, kind, src, dst, rows, peer):
        remote(
            wbuf.at[ch, src, rows], wbuf.at[ch, dst, rows],
            wss.at[0], wrs.at[ch, kind], peer,
        ).start()

    def step0(ch):
        wcopy(ch, 0, 0, 1, every, yp)
        wcopy(ch, 0, 0, 2, every, ym)
        wcopy(ch, 2, 0, 4, top, xp)
        wcopy(ch, 2, 0, 4, bottom, xm)

    def step1(ch):
        awaited(wbuf.at[ch, pl.ds(1, 2)], wrs.at[ch, 0])
        wcopy(ch, 1, 1, 3, top, yp)
        wcopy(ch, 1, 2, 3, bottom, ym)
        wcopy(ch, 2, pl.ds(1, 2), pl.ds(5, 2), top, xp)
        wcopy(ch, 2, pl.ds(1, 2), pl.ds(5, 2), bottom, xm)

    def step2(ch):
        awaited(wbuf.at[ch, 3], wrs.at[ch, 1])
        wcopy(ch, 2, 3, 7, top, xp)
        wcopy(ch, 2, 3, 7, bottom, xm)

    def step3(ch):
        awaited(wbuf.at[ch, pl.ds(4, 4)], wrs.at[ch, 2])

    def xstep1(ch):
        awaited(wbuf.at[ch, pl.ds(1, 2)], wrs.at[ch, 0])
        wcopy(ch, 1, 1, 3, top, yp)
        wcopy(ch, 1, 2, 3, bottom, ym)
        awaited(wbuf.at[ch, 4], wrs.at[ch, 2])
        wcopy(ch, 3, 4, 5, every, yp)
        wcopy(ch, 3, 4, 6, every, ym)

    def xstep2(ch):
        awaited(wbuf.at[ch, pl.ds(5, 2)], wrs.at[ch, 3])
        wcopy(ch, 4, 5, 7, top, yp)
        wcopy(ch, 4, 6, 7, bottom, ym)

    def xstep3(ch):
        awaited(wbuf.at[ch, 3], wrs.at[ch, 1])
        awaited(wbuf.at[ch, 7], wrs.at[ch, 4])

    def pass_on(ch, slots):
        ref = wbuf.at[ch, slots]
        remote(ref, ref, wcs.at[0], wrc.at[ch - OS], co).start()

    def give(ch):
        pass_on(ch, pl.ds(1, 3))
        step3(ch)
        pass_on(ch, pl.ds(4, 4))

    def hop(src, dst, half, peer):
        remote(
            kvbuf.at[src[0], src[1], half], kvbuf.at[dst[0], dst[1], half],
            kss.at[0], krs.at[dst[0], dst[1] // 2, half], peer,
        ).start()

    def hops(s, ab, half, first=False):
        for way, peer in ((0, zp), (1, zm)):
            src = (0, 2 * ab) if first else (s - 1, 2 * ab + way)
            hop(src, (s, 2 * ab + way), half, peer)

    def landed(s, ab, half):
        awaited(kvbuf.at[s, pl.ds(2 * ab, 2), half], krs.at[s, ab, half])

    def cross(g, js, k):
        ref = kvbuf.at[g, js]
        return remote(ref, ref, css.at[0], crs.at[g, k], co)

    def column(slot):
        yy = (y + (0, 3, 1, 2)[slot % 4]) % 4
        xx = xl if slot < 4 else 1 - xl
        return pl.ds(pl.multiple_of((yy * 2 + xx) * HD, HD), HD)

    def normalize():
        for copy in small:
            copy.wait()
        hidden = hid[...].astype(F32)
        inv = lax.rsqrt(jnp.mean(hidden * hidden, axis=-1, keepdims=True) + 1e-06)
        own = pl.ds(pl.multiple_of(c * ROWS, ROWS), ROWS)
        for slot in range(8):
            col = column(slot)
            part = hid[:, col].astype(F32) * inv * gain[:, col]
            nrel[own, slot * HD : (slot + 1) * HD] = part.astype(BF16)
        at = pl.ds(sq // 2, 1)
        cb, sb = cbase[at, :], sbase[at, :]
        cr, sr = crow[...], srow[...]
        cos[...] = cb * cr - sb * sr
        sin[...] = sb * cr + cb * sr
        acc[...] = jnp.zeros_like(acc)
        lrow[...] = jnp.zeros_like(lrow)
        mrow[...] = jnp.full_like(mrow, -1e30)

    def give_rows():
        own = pl.ds(pl.multiple_of(c * ROWS, ROWS), ROWS)
        remote(nrel.at[own], nrel.at[own], nss.at[0], nrs.at[0], co).start()

    def partner_rows():
        other = pl.ds(pl.multiple_of((1 - c) * ROWS, ROWS), ROWS)
        awaited(nrel.at[other], nrs.at[0])

    def projected(ch):
        w = wbuf[ch].reshape(8 * HD, HD)
        return jnp.dot(nrel[...], w, preferred_element_type=F32)

    def rotary(u):
        first, second = u[:, : HD // 2], u[:, HD // 2 :]
        cs, sn = cos[...], sin[...]
        return jnp.concatenate(
            [first * cs - second * sn, second * cs + first * sn], axis=1
        )

    def query(h):
        q = (rotary(projected(QS + h)) * HD ** (-0.5)).astype(BF16)
        qbuf[h] = q[:ROWS]
        qout[h] = q[ROWS:]
        remote(qout.at[h], qbuf.at[h], qss.at[0], qrs.at[0], co).start()

    def attend(g):
        online(kvbuf[g].reshape(8 * ROWS, 2 * HD))

    def attend_way(way):
        online(
            jnp.concatenate(
                [kvbuf[0, 2 * ab + way].reshape(2 * ROWS, 2 * HD) for ab in range(2)]
            )
        )

    def online(kv):
        keys, values = kv[:, :HD], kv[:, HD:]
        q = qbuf[...].reshape(HEADS * ROWS, HD)
        s = lax.dot_general(
            q, keys, (((1,), (1,)), ((), ())), preferred_element_type=F32
        )
        old = mrow[:, :1]
        new = jnp.maximum(old, jnp.max(s, axis=1, keepdims=True))
        scale = jnp.exp(old - new)
        e = jnp.exp(s - new)
        lrow[...] = lrow[...] * scale + jnp.sum(e, axis=1, keepdims=True)
        mrow[...] = jnp.broadcast_to(new, mrow.shape)
        acc[...] = acc[...] * scale + jnp.dot(
            e.astype(BF16), values, preferred_element_type=F32
        )

    def finish():
        att = (acc[...] / lrow[:, :1]).astype(BF16)
        total = jnp.zeros((ROWS, 1), F32)
        for slot in range(8):
            part = jnp.zeros((ROWS, HD), F32)
            for h in range(HEADS):
                part += jnp.dot(
                    att[h * ROWS : (h + 1) * ROWS], wbuf[OS + h, slot],
                    preferred_element_type=F32,
                )
            proj[:, slot * HD : (slot + 1) * HD] = part
            total += jnp.sum(part * part, axis=1, keepdims=True)
        inv = lax.rsqrt(total / (8 * HD) + 1e-06)
        for slot in range(8):
            col = column(slot)
            part = proj[:, slot * HD : (slot + 1) * HD] * inv * pgain[:, col]
            out[:, col] = (hid[:, col].astype(F32) + part).astype(BF16)

    @pl.when(c == 1)
    def _():
        awaited(wbuf.at[pl.ds(0, 2), 0], lsem.at[0])
        step0(0)
        step0(1)
        normalize()
        step1(0)
        give_rows()
        step1(1)
        step2(0)
        step2(1)
        partner_rows()
        step3(0)
        k = rotary(projected(0)).astype(BF16)
        kvbuf[0, 0, :, :, :HD] = k.reshape(PIECES, PIECE, HD)

        def first(cols):
            for half in range(PIECES):
                remote(
                    kvbuf.at[0, 0, half, :, cols], kvbuf.at[0, 2, half, :, cols],
                    xss.at[0], xrs.at[half], xo,
                ).start()
                for way, peer in ((0, zp), (1, zm)):
                    remote(
                        kvbuf.at[0, 0, half, :, cols], kvbuf.at[1, way, half, :, cols],
                        kss.at[0], krs.at[1, 0, half], peer,
                    ).start()

        first(pl.ds(0, HD))
        step3(1)
        v = projected(1).astype(BF16)
        kvbuf[0, 0, :, :, HD:] = v.reshape(PIECES, PIECE, HD)
        first(pl.ds(HD, HD))
        cross(0, 0, 0).start()

        def turn(s, ab):
            for half in range(PIECES):
                landed(s - 1, ab, half)
                hops(s, ab, half)

        turn(2, 0)
        for half in range(PIECES):
            awaited(kvbuf.at[0, 2, half], xrs.at[half])
            hops(1, 1, half, True)
        cross(0, 2, 1).start()

        def early(s, _):
            turn(s, 0)
            turn(s - 1, 1)
            cross(s - 2, pl.ds(0, 4), 0).start()
            return 0

        lax.fori_loop(3, 6, early, 0)

        turn(6, 0)
        turn(5, 1)
        cross(4, pl.ds(0, 4), 0).start()
        awaited(qbuf, qrs.at[0])
        attend_way(0)
        attend(1)
        turn(7, 0)
        attend(2)
        turn(6, 1)
        cross(5, pl.ds(0, 4), 0).start()
        attend(3)
        for half in range(PIECES):
            landed(HALF - 1, 0, half)
            hop((HALF - 1, 0), (0, 1), half, zp)
        attend(4)
        turn(7, 1)
        cross(6, pl.ds(0, 4), 0).start()
        attend(5)
        for half in range(PIECES):
            landed(HALF - 1, 1, half)
            hop((HALF - 1, 3), (0, 3), half, zm)
        cross(HALF - 1, pl.ds(0, 4), 0).start()
        attend(6)
        attend(7)
        for ab in range(2):
            for half in range(PIECES):
                awaited(kvbuf.at[0, 2 * ab + 1, half], krs.at[0, ab, half])
            cross(0, 2 * ab + 1, 2 + ab).start()
        attend_way(1)
        awaited(wbuf.at[pl.ds(OS, HEADS), 0], lsem.at[1])
        for ch in range(OS, NCH):
            awaited(wbuf.at[ch, pl.ds(1, 7)], wrc.at[ch - OS])
        finish()
        awaited(wbuf.at[pl.ds(0, 2), pl.ds(0, 7)], wss.at[0])
        awaited(wbuf.at[pl.ds(0, 6), pl.ds(0, 5)], kss.at[0])
        awaited(kvbuf.at[0, 0], xss.at[0])
        awaited(kvbuf, css.at[0])

    @pl.when(c == 0)
    def _():
        awaited(wbuf.at[pl.ds(QS, 2 * HEADS), 0], lsem.at[1])
        step0(2)
        normalize()
        give_rows()
        partner_rows()

        def near(g):
            awaited(kvbuf.at[g], crs.at[g, 0])
            attend(g)

        def near_own():
            for j, k in ((0, 0), (2, 1)):
                awaited(kvbuf.at[0, j], crs.at[0, k])
            attend_way(0)

        step0(3)
        step0(4)
        step1(2)
        step0(5)
        step1(3)
        step0(6)
        xstep1(4)
        step2(2)
        step0(7)
        step1(5)
        step2(3)
        step0(8)
        step1(6)
        xstep2(4)
        step0(9)
        step3(2)
        query(0)
        step1(7)
        step2(5)
        step0(10)
        step3(3)
        query(1)
        step1(8)
        step2(6)
        step0(11)
        xstep3(4)
        query(2)
        step1(9)
        step2(7)
        step3(5)
        query(3)
        step1(10)
        step2(8)
        step3(6)
        query(4)
        step1(11)
        step2(9)
        near_own()
        give(7)
        step2(10)
        near(1)
        give(8)
        step2(11)
        near(2)
        give(9)
        near(3)
        near(4)
        give(10)
        near(5)
        near(6)
        give(11)
        near(7)
        for j, k in ((1, 2), (3, 3)):
            awaited(kvbuf.at[0, j], crs.at[0, k])
        attend_way(1)
        finish()
        awaited(wbuf.at[pl.ds(QS, 2 * HEADS), pl.ds(0, 7)], wss.at[0])
        awaited(wbuf.at[pl.ds(OS, HEADS), pl.ds(1, 7)], wcs.at[0])
        awaited(qout, qss.at[0])

    own = pl.ds(pl.multiple_of(c * ROWS, ROWS), ROWS)
    awaited(nrel.at[own], nss.at[0])


def local(hidden_in, attn_gain, w_query, w_keyval, w_output, post_gain):
    count, width = hidden_in.shape[1:]
    freq = 10000.0 ** (-np.arange(HD // 2) * 2.0 / HD)
    row = np.arange(2 * ROWS)[:, None] * freq
    base = np.arange(2 * NZ)[:, None] * (2 * ROWS) * freq
    tables = [np.asarray(f(a), np.float32) for a in (row, base) for f in (np.cos, np.sin)]
    vmem = pl.BlockSpec(memory_space=pltpu.VMEM)
    hbm = pl.BlockSpec(memory_space=pl.ANY)
    dma = pltpu.SemaphoreType.DMA
    operands = [
        hidden_in[0], attn_gain[None], *tables, post_gain[None],
        w_query, w_keyval, w_output,
    ]
    result = pl.pallas_call(
        ring_kernel,
        out_shape=jax.ShapeDtypeStruct((count, width), BF16),
        in_specs=[hbm] * 10,
        out_specs=vmem,
        scratch_shapes=[
            pltpu.VMEM((count, width), BF16),
            pltpu.VMEM((1, width), F32),
            pltpu.VMEM((2 * ROWS, HD // 2), F32),
            pltpu.VMEM((2 * ROWS, HD // 2), F32),
            pltpu.VMEM((2 * NZ, HD // 2), F32),
            pltpu.VMEM((2 * NZ, HD // 2), F32),
            pltpu.VMEM((1, width), F32),
            pltpu.VMEM((NCH, 8, HD, HD), BF16),
            pltpu.VMEM((HALF, 4, PIECES, PIECE, 2 * HD), BF16),
            pltpu.VMEM((2 * ROWS, 8 * HD), BF16),
            pltpu.VMEM((HEADS, ROWS, HD), BF16),
            pltpu.VMEM((HEADS, ROWS, HD), BF16),
            pltpu.VMEM((HEADS * ROWS, HD), F32),
            pltpu.VMEM((HEADS * ROWS, 128), F32),
            pltpu.VMEM((HEADS * ROWS, 128), F32),
            pltpu.VMEM((ROWS, 8 * HD), F32),
            pltpu.VMEM((2 * ROWS, HD // 2), F32),
            pltpu.VMEM((2 * ROWS, HD // 2), F32),
            dma((9,)),
            dma((1,)),
            dma((1,)),
            dma((NCH, 5)),
            dma((HEADS,)),
            dma((HALF, 2, PIECES)),
            dma((1,)),
            dma((1,)),
            dma((PIECES,)),
            dma((1,)),
            dma((HALF, 4)),
            dma((1,)),
            dma((1,)),
            dma((1,)),
            dma((1,)),
        ],
        compiler_params=pltpu.CompilerParams(
            collective_id=0, has_side_effects=True, vmem_limit_bytes=40 * 1024 * 1024
        ),
    )(
        *(pltpu.with_memory_space_constraint(a, pltpu.HBM) for a in operands)
    )
    return result[None]


def solution(mesh):
    return jax.shard_map(
        local,
        mesh=mesh,
        in_specs=(
            P("dp", "seq", None), P(), P("dp", None), P("dp", None), P(None, "dp"), P(),
        ),
        out_specs=P("dp", "seq", None),
        check_vma=False,
    )
```

```python
import jax
import jax.numpy as jnp
import numpy as np
from jax import lax
from jax.experimental import pallas as pl
from jax.experimental.pallas import tpu as pltpu
from jax.sharding import PartitionSpec as P

BF16 = jnp.bfloat16
F32 = jnp.float32

ROWS = 64
HD = 256
HEADS = 5
QS, OS = 2, 2 + HEADS
NCH = OS + HEADS
NZ = 16
HALF = NZ // 2
PIECES = 4
MESH = pl.DeviceIdType.MESH


def ring_kernel(
    hid_in, gain_in, crow_in, srow_in, cbase_in, sbase_in, pgain_in, wq, wkv, wo, out,
    hid, gain, crow, srow, cbase, sbase, pgain, wbuf, kvbuf, nrel, qbuf, qout, acc, mrow, lrow, proj, cos, sin, ebuf, sbuf,
    lsem, wss, wcs, wrs, wrc, krs, kss, xss, xrs, css, crs, nss, nrs, qss, qrs,
):
    dp = lax.axis_index("dp")
    sq = lax.axis_index("seq")
    y, xl = dp // 2, dp % 2
    xh, z, c = sq // 32, (sq // 2) % NZ, sq % 2

    def dev(yy, xll, xhh, zz, cc):
        return (yy * 2 + xll, xhh * 32 + zz * 2 + cc)

    yp = dev((y + 1) % 4, xl, xh, z, c)
    ym = dev((y + 3) % 4, xl, xh, z, c)
    xp = dev(y, 1 - xl, (xh + xl) % 2, z, c)
    xm = dev(y, 1 - xl, (xh + 1 - xl) % 2, z, c)
    xo = dev(y, xl, 1 - xh, z, c)
    zp = dev(y, xl, xh, (z + 1) % NZ, c)
    zm = dev(y, xl, xh, (z + NZ - 1) % NZ, c)
    co = dev(y, xl, xh, z, 1 - c)

    def remote(src, dst, ssem, rsem, peer):
        return pltpu.make_async_remote_copy(
            src_ref=src, dst_ref=dst, send_sem=ssem, recv_sem=rsem,
            device_id=peer, device_id_type=MESH,
        )

    def awaited(ref, sem):
        pltpu.make_async_copy(ref, ref, sem).wait()

    barrier = pltpu.get_barrier_semaphore()
    for peer in (yp, ym, xp, xm, xo, zp, zm, co):
        pl.semaphore_signal(barrier, inc=1, device_id=peer, device_id_type=MESH)

    def load(ch):
        if ch < QS:
            src = wkv.at[:, pl.ds(ch * HD, HD)]
        elif ch < OS:
            src = wq.at[:, pl.ds((ch - QS) * HD, HD)]
        else:
            src = wo.at[pl.ds((ch - OS) * HD, HD), :]
        sem = lsem.at[0 if ch < QS else 1]
        pltpu.make_async_copy(src, wbuf.at[ch, 0], sem).start()

    small = [
        pltpu.make_async_copy(src, dst, lsem.at[2 + i])
        for i, (src, dst) in enumerate(
            [
                (hid_in, hid), (gain_in, gain), (crow_in, crow), (srow_in, srow),
                (cbase_in, cbase), (sbase_in, sbase), (pgain_in, pgain),
            ]
        )
    ]

    @pl.when(c == 1)
    def _():
        for ch in (0, 1):
            load(ch)

    for copy in small:
        copy.start()

    @pl.when(c == 1)
    def _():
        for ch in range(OS, NCH):
            load(ch)

    @pl.when(c == 0)
    def _():
        for ch in range(QS, NCH):
            load(ch)

    pl.semaphore_wait(barrier, 8)

    top, bottom, every = pl.ds(0, 128), pl.ds(128, 128), pl.ds(0, 256)

    def wcopy(ch, kind, src, dst, rows, peer):
        remote(
            wbuf.at[ch, src, rows], wbuf.at[ch, dst, rows],
            wss.at[0], wrs.at[ch, kind], peer,
        ).start()

    def own_y(ch):
        wcopy(ch, 0, 0, 1, every, yp)
        wcopy(ch, 0, 0, 2, every, ym)

    def own_x(ch):
        wcopy(ch, 2, 0, 4, top, xp)
        wcopy(ch, 2, 0, 4, bottom, xm)

    def step0(ch):
        own_y(ch)
        own_x(ch)

    def step1(ch):
        awaited(wbuf.at[ch, pl.ds(1, 2)], wrs.at[ch, 0])
        wcopy(ch, 1, 1, 3, top, yp)
        wcopy(ch, 1, 2, 3, bottom, ym)
        wcopy(ch, 2, pl.ds(1, 2), pl.ds(5, 2), top, xp)
        wcopy(ch, 2, pl.ds(1, 2), pl.ds(5, 2), bottom, xm)

    def step2(ch):
        awaited(wbuf.at[ch, 3], wrs.at[ch, 1])
        wcopy(ch, 2, 3, 7, top, xp)
        wcopy(ch, 2, 3, 7, bottom, xm)

    def step3(ch):
        awaited(wbuf.at[ch, pl.ds(4, 4)], wrs.at[ch, 2])

    def xstep1(ch):
        awaited(wbuf.at[ch, pl.ds(1, 2)], wrs.at[ch, 0])
        wcopy(ch, 1, 1, 3, top, yp)
        wcopy(ch, 1, 2, 3, bottom, ym)
        awaited(wbuf.at[ch, 4], wrs.at[ch, 2])
        wcopy(ch, 3, 4, 5, every, yp)
        wcopy(ch, 3, 4, 6, every, ym)

    def xstep2(ch):
        awaited(wbuf.at[ch, pl.ds(5, 2)], wrs.at[ch, 3])
        wcopy(ch, 4, 5, 7, top, yp)
        wcopy(ch, 4, 6, 7, bottom, ym)

    def xstep3(ch):
        awaited(wbuf.at[ch, 3], wrs.at[ch, 1])
        awaited(wbuf.at[ch, 7], wrs.at[ch, 4])

    def pass_on(ch, slots):
        ref = wbuf.at[ch, slots]
        remote(ref, ref, wcs.at[0], wrc.at[ch - OS], co).start()

    def give(ch):
        pass_on(ch, pl.ds(1, 3))
        step3(ch)
        pass_on(ch, pl.ds(4, 4))

    def hop(src, dst, half, peer):
        remote(
            kvbuf.at[src[0], src[1], half], kvbuf.at[dst[0], dst[1], half],
            kss.at[0], krs.at[dst[0], dst[1] // 2, half], peer,
        ).start()

    def hops(s, ab, half, first=False):
        for way, peer in ((0, zp), (1, zm)):
            src = (0, 2 * ab) if first else (s - 1, 2 * ab + way)
            hop(src, (s, 2 * ab + way), half, peer)

    def landed(s, ab, half):
        awaited(kvbuf.at[s, pl.ds(2 * ab, 2), half], krs.at[s, ab, half])

    def cross(g, js, k):
        ref = kvbuf.at[g, js]
        return remote(ref, ref, css.at[0], crs.at[g, k], co)

    def column(slot):
        yy = (y + (0, 3, 1, 2)[slot % 4]) % 4
        xx = xl if slot < 4 else 1 - xl
        return pl.ds(pl.multiple_of((yy * 2 + xx) * HD, HD), HD)

    def normalize():
        for copy in small:
            copy.wait()
        hidden = hid[...].astype(F32)
        inv = lax.rsqrt(jnp.mean(hidden * hidden, axis=-1, keepdims=True) + 1e-06)
        own = pl.ds(pl.multiple_of(c * ROWS, ROWS), ROWS)
        for slot in range(8):
            col = column(slot)
            part = hid[:, col].astype(F32) * inv * gain[:, col]
            nrel[own, slot * HD : (slot + 1) * HD] = part.astype(BF16)
        at = pl.ds(sq // 2, 1)
        cb, sb = cbase[at, :], sbase[at, :]
        cr, sr = crow[...], srow[...]
        cos[...] = cb * cr - sb * sr
        sin[...] = sb * cr + cb * sr
        acc[...] = jnp.zeros_like(acc)
        lrow[...] = jnp.zeros_like(lrow)
        mrow[...] = jnp.full_like(mrow, -1e30)

    def give_rows():
        own = pl.ds(pl.multiple_of(c * ROWS, ROWS), ROWS)
        remote(nrel.at[own], nrel.at[own], nss.at[0], nrs.at[0], co).start()

    def partner_rows():
        other = pl.ds(pl.multiple_of((1 - c) * ROWS, ROWS), ROWS)
        awaited(nrel.at[other], nrs.at[0])

    def projected(ch):
        w = wbuf[ch].reshape(8 * HD, HD)
        return jnp.dot(nrel[...], w, preferred_element_type=F32)

    def rotary(u):
        first, second = u[:, : HD // 2], u[:, HD // 2 :]
        cs, sn = cos[...], sin[...]
        return jnp.concatenate(
            [first * cs - second * sn, second * cs + first * sn], axis=1
        )

    def query(h):
        q = (rotary(projected(QS + h)) * HD ** (-0.5)).astype(BF16)
        qbuf[h] = q[:ROWS]
        qout[h] = q[ROWS:]
        remote(qout.at[h], qbuf.at[h], qss.at[0], qrs.at[0], co).start()

    def group(g):
        return tuple(
            kvbuf[g, :, 2 * i : 2 * i + 2].reshape(8 * ROWS, HD) for i in range(2)
        )

    def group_way(way):
        return tuple(
            jnp.concatenate(
                [
                    kvbuf[0, 2 * ab + way, 2 * i : 2 * i + 2].reshape(2 * ROWS, HD)
                    for ab in range(2)
                ]
            )
            for i in range(2)
        )

    def weigh(kv):
        q = qbuf[...].reshape(HEADS * ROWS, HD)
        s = lax.dot_general(
            q, kv[0], (((1,), (1,)), ((), ())), preferred_element_type=F32
        )
        old = mrow[:, :1]
        new = jnp.maximum(old, jnp.max(s, axis=1, keepdims=True))
        scale = jnp.exp(old - new)
        e = jnp.exp(s - new)
        lrow[...] = lrow[...] * scale + jnp.sum(e, axis=1, keepdims=True)
        mrow[...] = jnp.broadcast_to(new, mrow.shape)
        return e.astype(BF16), scale

    def gather(e, scale, kv):
        acc[...] = acc[...] * scale + jnp.dot(
            e, kv[1], preferred_element_type=F32
        )

    def online(kv):
        e, scale = weigh(kv)
        gather(e, scale, kv)

    def attend(g):
        online(group(g))

    def attend_way(way):
        online(group_way(way))

    def halves(kv):
        def early():
            e, scale = weigh(kv())
            ebuf[:, : e.shape[1]] = e
            sbuf[...] = jnp.broadcast_to(scale, sbuf.shape)

        def late():
            v = kv()
            gather(ebuf[:, : v[1].shape[0]], sbuf[:, :1], v)

        return early, late

    def finish():
        att = (acc[...] / lrow[:, :1]).astype(BF16)
        total = jnp.zeros((ROWS, 1), F32)
        for slot in range(8):
            part = jnp.zeros((ROWS, HD), F32)
            for h in range(HEADS):
                part += jnp.dot(
                    att[h * ROWS : (h + 1) * ROWS], wbuf[OS + h, slot],
                    preferred_element_type=F32,
                )
            proj[:, slot * HD : (slot + 1) * HD] = part
            total += jnp.sum(part * part, axis=1, keepdims=True)
        inv = lax.rsqrt(total / (8 * HD) + 1e-06)
        for slot in range(8):
            col = column(slot)
            part = proj[:, slot * HD : (slot + 1) * HD] * inv * pgain[:, col]
            out[:, col] = (hid[:, col].astype(F32) + part).astype(BF16)

    @pl.when(c == 1)
    def _():
        awaited(wbuf.at[pl.ds(0, 2), 0], lsem.at[0])
        step0(0)
        step0(1)
        normalize()
        give_rows()
        step1(0)
        step1(1)
        step2(0)
        step2(1)
        partner_rows()
        step3(0)
        def first(part, u):
            kvbuf[0, 0, 2 * part : 2 * part + 2] = u.astype(BF16).reshape(2, ROWS, HD)
            for half in range(2 * part, 2 * part + 2):
                remote(
                    kvbuf.at[0, 0, half], kvbuf.at[0, 2, half],
                    xss.at[0], xrs.at[half], xo,
                ).start()
                hops(1, 0, half, True)

        first(0, rotary(projected(0)))
        step3(1)
        first(1, projected(1))
        cross(0, 0, 0).start()

        def between(half, work):
            if work and half % (PIECES // 2) == PIECES // 2 - 1:
                work[half // (PIECES // 2)]()

        def turn(s, ab, work=None):
            for half in range(PIECES):
                landed(s - 1, ab, half)
                hops(s, ab, half)
                between(half, work)

        turn(2, 0)
        for half in range(PIECES):
            awaited(kvbuf.at[0, 2, half], xrs.at[half])
            hops(1, 1, half, True)
        cross(0, 2, 1).start()

        def early(s, _):
            turn(s, 0)
            turn(s - 1, 1)
            cross(s - 2, pl.ds(0, 4), 0).start()
            return 0

        lax.fori_loop(3, 6, early, 0)

        turn(6, 0)
        turn(5, 1)
        cross(4, pl.ds(0, 4), 0).start()
        turn(7, 0)
        awaited(qbuf, qrs.at[0])
        turn(6, 1, halves(lambda: group(1)))
        cross(5, pl.ds(0, 4), 0).start()
        work = halves(lambda: group(2))
        for half in range(PIECES):
            landed(HALF - 1, 0, half)
            hop((HALF - 1, half % 2), (0, 1), half, (zp, zm)[half % 2])
            between(half, work)
        cross(HALF - 1, pl.ds(0, 2), 0).start()
        turn(7, 1, halves(lambda: group(3)))
        cross(6, pl.ds(0, 4), 0).start()
        work = halves(lambda: group(4))
        for half in range(PIECES):
            landed(HALF - 1, 1, half)
            hop((HALF - 1, 2 + half % 2), (0, 3), half, (zp, zm)[half % 2])
            between(half, work)
        cross(HALF - 1, pl.ds(2, 2), 1).start()
        attend(5)
        attend_way(0)
        attend(6)
        attend(7)
        for ab in range(2):
            for half in range(PIECES):
                awaited(kvbuf.at[0, 2 * ab + 1, half], krs.at[0, ab, half])
            cross(0, 2 * ab + 1, 2 + ab).start()
        attend_way(1)
        awaited(wbuf.at[pl.ds(OS, HEADS), 0], lsem.at[1])
        for ch in range(OS, NCH):
            awaited(wbuf.at[ch, pl.ds(1, 7)], wrc.at[ch - OS])
        finish()
        awaited(wbuf.at[pl.ds(0, 2), pl.ds(0, 7)], wss.at[0])
        awaited(wbuf.at[pl.ds(0, 6), pl.ds(0, 5)], kss.at[0])
        awaited(kvbuf.at[0, 0], xss.at[0])
        awaited(kvbuf, css.at[0])

    @pl.when(c == 0)
    def _():
        awaited(wbuf.at[pl.ds(QS, 2 * HEADS), 0], lsem.at[1])
        own_x(2)
        own_x(3)
        own_x(4)
        own_x(5)
        own_x(6)
        normalize()
        give_rows()
        partner_rows()

        def near(g):
            awaited(kvbuf.at[g], crs.at[g, 0])
            attend(g)

        def near_own():
            for j, k in ((0, 0), (2, 1)):
                awaited(kvbuf.at[0, j], crs.at[0, k])
            attend_way(0)

        own_y(2)
        step1(2)
        own_y(3)
        own_y(4)
        own_y(5)
        step1(3)
        own_y(6)
        xstep1(4)
        step2(2)
        step0(7)
        step1(5)
        step2(3)
        step0(8)
        step1(6)
        xstep2(4)
        step0(9)
        step3(2)
        query(0)
        step1(7)
        step2(5)
        step0(10)
        step3(3)
        query(1)
        step1(8)
        step2(6)
        step0(11)
        xstep3(4)
        query(2)
        step1(9)
        step2(7)
        step3(5)
        query(3)
        step1(10)
        step2(8)
        step3(6)
        query(4)
        step1(11)
        step2(9)
        near_own()
        give(7)
        step2(10)
        near(1)
        give(8)
        step2(11)
        near(2)
        give(9)
        near(3)
        near(4)
        give(10)
        near(5)
        near(6)
        give(11)
        awaited(kvbuf.at[HALF - 1, pl.ds(0, 2)], crs.at[HALF - 1, 0])
        awaited(kvbuf.at[HALF - 1, pl.ds(2, 2)], crs.at[HALF - 1, 1])
        attend(7)
        for j, k in ((1, 2), (3, 3)):
            awaited(kvbuf.at[0, j], crs.at[0, k])
        attend_way(1)
        finish()
        awaited(wbuf.at[pl.ds(QS, 2 * HEADS), pl.ds(0, 7)], wss.at[0])
        awaited(wbuf.at[pl.ds(OS, HEADS), pl.ds(1, 7)], wcs.at[0])
        awaited(qout, qss.at[0])

    own = pl.ds(pl.multiple_of(c * ROWS, ROWS), ROWS)
    awaited(nrel.at[own], nss.at[0])


def local(hidden_in, attn_gain, w_query, w_keyval, w_output, post_gain):
    count, width = hidden_in.shape[1:]
    freq = 10000.0 ** (-np.arange(HD // 2) * 2.0 / HD)
    row = np.arange(2 * ROWS)[:, None] * freq
    base = np.arange(2 * NZ)[:, None] * (2 * ROWS) * freq
    tables = [np.asarray(f(a), np.float32) for a in (row, base) for f in (np.cos, np.sin)]
    vmem = pl.BlockSpec(memory_space=pltpu.VMEM)
    hbm = pl.BlockSpec(memory_space=pl.ANY)
    dma = pltpu.SemaphoreType.DMA
    operands = [
        hidden_in[0], attn_gain[None], *tables, post_gain[None],
        w_query, w_keyval, w_output,
    ]
    result = pl.pallas_call(
        ring_kernel,
        out_shape=jax.ShapeDtypeStruct((count, width), BF16),
        in_specs=[hbm] * 10,
        out_specs=vmem,
        scratch_shapes=[
            pltpu.VMEM((count, width), BF16),
            pltpu.VMEM((1, width), F32),
            pltpu.VMEM((2 * ROWS, HD // 2), F32),
            pltpu.VMEM((2 * ROWS, HD // 2), F32),
            pltpu.VMEM((2 * NZ, HD // 2), F32),
            pltpu.VMEM((2 * NZ, HD // 2), F32),
            pltpu.VMEM((1, width), F32),
            pltpu.VMEM((NCH, 8, HD, HD), BF16),
            pltpu.VMEM((HALF, 4, PIECES, ROWS, HD), BF16),
            pltpu.VMEM((2 * ROWS, 8 * HD), BF16),
            pltpu.VMEM((HEADS, ROWS, HD), BF16),
            pltpu.VMEM((HEADS, ROWS, HD), BF16),
            pltpu.VMEM((HEADS * ROWS, HD), F32),
            pltpu.VMEM((HEADS * ROWS, 128), F32),
            pltpu.VMEM((HEADS * ROWS, 128), F32),
            pltpu.VMEM((ROWS, 8 * HD), F32),
            pltpu.VMEM((2 * ROWS, HD // 2), F32),
            pltpu.VMEM((2 * ROWS, HD // 2), F32),
            pltpu.VMEM((HEADS * ROWS, 8 * ROWS), BF16),
            pltpu.VMEM((HEADS * ROWS, 128), F32),
            dma((9,)),
            dma((1,)),
            dma((1,)),
            dma((NCH, 5)),
            dma((HEADS,)),
            dma((HALF, 2, PIECES)),
            dma((1,)),
            dma((1,)),
            dma((PIECES,)),
            dma((1,)),
            dma((HALF, 4)),
            dma((1,)),
            dma((1,)),
            dma((1,)),
            dma((1,)),
        ],
        compiler_params=pltpu.CompilerParams(
            collective_id=0, has_side_effects=True, vmem_limit_bytes=40 * 1024 * 1024
        ),
    )(
        *(pltpu.with_memory_space_constraint(a, pltpu.HBM) for a in operands)
    )
    return result[None]


def solution(mesh):
    return jax.shard_map(
        local,
        mesh=mesh,
        in_specs=(
            P("dp", "seq", None), P(), P("dp", None), P("dp", None), P(None, "dp"), P(),
        ),
        out_specs=P("dp", "seq", None),
        check_vma=False,
    )
```

```python
import jax
import jax.numpy as jnp
import numpy as np
from jax import lax
from jax.experimental import pallas as pl
from jax.experimental.pallas import tpu as pltpu
from jax.sharding import PartitionSpec as P

BF16 = jnp.bfloat16
F32 = jnp.float32

ROWS = 64
HD = 256
HEADS = 5
QS, OS = 2, 2 + HEADS
NCH = OS + HEADS
NZ = 16
HALF = NZ // 2
PIECES = 4
MESH = pl.DeviceIdType.MESH


def ring_kernel(
    hid_in, gain_in, crow_in, srow_in, cbase_in, sbase_in, pgain_in, wq, wkv, wo, out,
    hid, gain, crow, srow, cbase, sbase, pgain, wbuf, kvbuf, nrel, qbuf, qout, acc, mrow, lrow, proj, cos, sin, ebuf, sbuf,
    lsem, wss, wcs, wrs, wrc, krs, kss, xss, xrs, css, crs, nss, nrs, qss, qrs,
):
    dp = lax.axis_index("dp")
    sq = lax.axis_index("seq")
    y, xl = dp // 2, dp % 2
    xh, z, c = sq // 32, (sq // 2) % NZ, sq % 2

    def dev(yy, xll, xhh, zz, cc):
        return (yy * 2 + xll, xhh * 32 + zz * 2 + cc)

    yp = dev((y + 1) % 4, xl, xh, z, c)
    ym = dev((y + 3) % 4, xl, xh, z, c)
    xp = dev(y, 1 - xl, (xh + xl) % 2, z, c)
    xm = dev(y, 1 - xl, (xh + 1 - xl) % 2, z, c)
    xo = dev(y, xl, 1 - xh, z, c)
    zp = dev(y, xl, xh, (z + 1) % NZ, c)
    zm = dev(y, xl, xh, (z + NZ - 1) % NZ, c)
    co = dev(y, xl, xh, z, 1 - c)

    def remote(src, dst, ssem, rsem, peer):
        return pltpu.make_async_remote_copy(
            src_ref=src, dst_ref=dst, send_sem=ssem, recv_sem=rsem,
            device_id=peer, device_id_type=MESH,
        )

    def awaited(ref, sem):
        pltpu.make_async_copy(ref, ref, sem).wait()

    barrier = pltpu.get_barrier_semaphore()
    for peer in (yp, ym, xp, xm, xo, zp, zm, co):
        pl.semaphore_signal(barrier, inc=1, device_id=peer, device_id_type=MESH)

    def load(ch):
        if ch < QS:
            src = wkv.at[:, pl.ds(ch * HD, HD)]
        elif ch < OS:
            src = wq.at[:, pl.ds((ch - QS) * HD, HD)]
        else:
            src = wo.at[pl.ds((ch - OS) * HD, HD), :]
        sem = lsem.at[0 if ch < QS else 1]
        pltpu.make_async_copy(src, wbuf.at[ch, 0], sem).start()

    small = [
        pltpu.make_async_copy(src, dst, lsem.at[2 + i])
        for i, (src, dst) in enumerate(
            [
                (hid_in, hid), (gain_in, gain), (crow_in, crow), (srow_in, srow),
                (cbase_in, cbase), (sbase_in, sbase), (pgain_in, pgain),
            ]
        )
    ]

    @pl.when(c == 1)
    def _():
        for ch in (0, 1):
            load(ch)

    for copy in small:
        copy.start()

    @pl.when(c == 1)
    def _():
        for ch in range(OS, NCH):
            load(ch)

    @pl.when(c == 0)
    def _():
        for ch in range(QS, NCH):
            load(ch)

    pl.semaphore_wait(barrier, 8)

    top, bottom, every = pl.ds(0, 128), pl.ds(128, 128), pl.ds(0, 256)

    def wcopy(ch, kind, src, dst, rows, peer):
        remote(
            wbuf.at[ch, src, rows], wbuf.at[ch, dst, rows],
            wss.at[0], wrs.at[ch, kind], peer,
        ).start()

    def own_y(ch):
        wcopy(ch, 0, 0, 1, every, yp)
        wcopy(ch, 0, 0, 2, every, ym)

    def own_x(ch):
        wcopy(ch, 2, 0, 4, top, xp)
        wcopy(ch, 2, 0, 4, bottom, xm)

    def step0(ch):
        own_y(ch)
        own_x(ch)

    def first0(ch):
        for kind, up, down in ((0, top, bottom), (5, bottom, top)):
            wcopy(ch, kind, 0, 1, up, yp)
            wcopy(ch, kind, 0, 2, down, ym)
        own_x(ch)

    def first1(ch):
        awaited(wbuf.at[ch, 1], wrs.at[ch, 0])
        wcopy(ch, 1, 1, 3, top, yp)
        wcopy(ch, 1, 2, 3, bottom, ym)
        wcopy(ch, 2, 1, 5, top, xp)
        wcopy(ch, 2, 2, 6, bottom, xm)

    def second1(ch):
        awaited(wbuf.at[ch, 2], wrs.at[ch, 5])
        wcopy(ch, 2, 2, 6, top, xp)
        wcopy(ch, 2, 1, 5, bottom, xm)

    def step1(ch):
        awaited(wbuf.at[ch, pl.ds(1, 2)], wrs.at[ch, 0])
        wcopy(ch, 1, 1, 3, top, yp)
        wcopy(ch, 1, 2, 3, bottom, ym)
        wcopy(ch, 2, pl.ds(1, 2), pl.ds(5, 2), top, xp)
        wcopy(ch, 2, pl.ds(1, 2), pl.ds(5, 2), bottom, xm)

    def step2(ch):
        awaited(wbuf.at[ch, 3], wrs.at[ch, 1])
        wcopy(ch, 2, 3, 7, top, xp)
        wcopy(ch, 2, 3, 7, bottom, xm)

    def step3(ch):
        awaited(wbuf.at[ch, pl.ds(4, 4)], wrs.at[ch, 2])

    def xstep1(ch):
        awaited(wbuf.at[ch, pl.ds(1, 2)], wrs.at[ch, 0])
        wcopy(ch, 1, 1, 3, top, yp)
        wcopy(ch, 1, 2, 3, bottom, ym)
        awaited(wbuf.at[ch, 4], wrs.at[ch, 2])
        wcopy(ch, 3, 4, 5, every, yp)
        wcopy(ch, 3, 4, 6, every, ym)

    def xstep2(ch):
        awaited(wbuf.at[ch, pl.ds(5, 2)], wrs.at[ch, 3])
        wcopy(ch, 4, 5, 7, top, yp)
        wcopy(ch, 4, 6, 7, bottom, ym)

    def xstep3(ch):
        awaited(wbuf.at[ch, 3], wrs.at[ch, 1])
        awaited(wbuf.at[ch, 7], wrs.at[ch, 4])

    def pass_on(ch, slots):
        ref = wbuf.at[ch, slots]
        remote(ref, ref, wcs.at[0], wrc.at[ch - OS], co).start()

    def give(ch):
        pass_on(ch, pl.ds(1, 3))
        step3(ch)
        pass_on(ch, pl.ds(4, 4))

    def hop(src, dst, half, peer):
        remote(
            kvbuf.at[src[0], src[1], half], kvbuf.at[dst[0], dst[1], half],
            kss.at[0], krs.at[dst[0], dst[1] // 2, half], peer,
        ).start()

    def hops(s, ab, half, first=False):
        for way, peer in ((0, zp), (1, zm)):
            src = (0, 2 * ab) if first else (s - 1, 2 * ab + way)
            hop(src, (s, 2 * ab + way), half, peer)

    def landed(s, ab, half):
        awaited(kvbuf.at[s, pl.ds(2 * ab, 2), half], krs.at[s, ab, half])

    def cross(g, js, k):
        ref = kvbuf.at[g, js]
        return remote(ref, ref, css.at[0], crs.at[g, k], co)

    def column(slot):
        yy = (y + (0, 3, 1, 2)[slot % 4]) % 4
        xx = xl if slot < 4 else 1 - xl
        return pl.ds(pl.multiple_of((yy * 2 + xx) * HD, HD), HD)

    def normalize():
        for copy in small:
            copy.wait()
        hidden = hid[...].astype(F32)
        inv = lax.rsqrt(jnp.mean(hidden * hidden, axis=-1, keepdims=True) + 1e-06)
        own = pl.ds(pl.multiple_of(c * ROWS, ROWS), ROWS)
        for slot in range(8):
            col = column(slot)
            part = hid[:, col].astype(F32) * inv * gain[:, col]
            nrel[own, slot * HD : (slot + 1) * HD] = part.astype(BF16)
        at = pl.ds(sq // 2, 1)
        cb, sb = cbase[at, :], sbase[at, :]
        cr, sr = crow[...], srow[...]
        cos[...] = cb * cr - sb * sr
        sin[...] = sb * cr + cb * sr
        acc[...] = jnp.zeros_like(acc)
        lrow[...] = jnp.zeros_like(lrow)
        mrow[...] = jnp.full_like(mrow, -1e30)

    def give_rows():
        own = pl.ds(pl.multiple_of(c * ROWS, ROWS), ROWS)
        remote(nrel.at[own], nrel.at[own], nss.at[0], nrs.at[0], co).start()

    def partner_rows():
        other = pl.ds(pl.multiple_of((1 - c) * ROWS, ROWS), ROWS)
        awaited(nrel.at[other], nrs.at[0])

    def projected(ch):
        w = wbuf[ch].reshape(8 * HD, HD)
        return jnp.dot(nrel[...], w, preferred_element_type=F32)

    def rotary(u):
        first, second = u[:, : HD // 2], u[:, HD // 2 :]
        cs, sn = cos[...], sin[...]
        return jnp.concatenate(
            [first * cs - second * sn, second * cs + first * sn], axis=1
        )

    def query(h):
        q = (rotary(projected(QS + h)) * HD ** (-0.5)).astype(BF16)
        qbuf[h] = q[:ROWS]
        qout[h] = q[ROWS:]
        remote(qout.at[h], qbuf.at[h], qss.at[0], qrs.at[0], co).start()

    def group(g):
        return tuple(
            kvbuf[g, :, 2 * i : 2 * i + 2].reshape(8 * ROWS, HD) for i in range(2)
        )

    def group_way(way):
        return tuple(
            jnp.concatenate(
                [
                    kvbuf[0, 2 * ab + way, 2 * i : 2 * i + 2].reshape(2 * ROWS, HD)
                    for ab in range(2)
                ]
            )
            for i in range(2)
        )

    def weigh(kv):
        q = qbuf[...].reshape(HEADS * ROWS, HD)
        s = lax.dot_general(
            q, kv[0], (((1,), (1,)), ((), ())), preferred_element_type=F32
        )
        old = mrow[:, :1]
        new = jnp.maximum(old, jnp.max(s, axis=1, keepdims=True))
        scale = jnp.exp(old - new)
        e = jnp.exp(s - new)
        lrow[...] = lrow[...] * scale + jnp.sum(e, axis=1, keepdims=True)
        mrow[...] = jnp.broadcast_to(new, mrow.shape)
        return e.astype(BF16), scale

    def gather(e, scale, kv):
        acc[...] = acc[...] * scale + jnp.dot(
            e, kv[1], preferred_element_type=F32
        )

    def online(kv):
        e, scale = weigh(kv)
        gather(e, scale, kv)

    def attend(g):
        online(group(g))

    def attend_way(way):
        online(group_way(way))

    def halves(kv):
        def early():
            e, scale = weigh(kv())
            ebuf[:, : e.shape[1]] = e
            sbuf[...] = jnp.broadcast_to(scale, sbuf.shape)

        def late():
            v = kv()
            gather(ebuf[:, : v[1].shape[0]], sbuf[:, :1], v)

        return early, late

    def finish():
        heads = (acc[...] / lrow[:, :1]).astype(BF16)
        att = jnp.concatenate(
            [heads[h * ROWS : (h + 1) * ROWS] for h in range(HEADS)], axis=1
        )
        total = jnp.zeros((ROWS, 1), F32)
        for slot in range(8):
            w = wbuf[OS:, slot].reshape(HEADS * HD, HD)
            part = jnp.dot(att, w, preferred_element_type=F32)
            proj[:, slot * HD : (slot + 1) * HD] = part
            total += jnp.sum(part * part, axis=1, keepdims=True)
        inv = lax.rsqrt(total / (8 * HD) + 1e-06)
        for slot in range(8):
            col = column(slot)
            part = proj[:, slot * HD : (slot + 1) * HD] * inv * pgain[:, col]
            out[:, col] = (hid[:, col].astype(F32) + part).astype(BF16)

    @pl.when(c == 1)
    def _():
        awaited(wbuf.at[pl.ds(0, 2), 0], lsem.at[0])
        first0(0)
        first0(1)
        normalize()
        give_rows()
        first1(0)
        second1(0)
        first1(1)
        second1(1)
        step2(0)
        step2(1)
        partner_rows()
        step3(0)
        def first(part, u):
            kvbuf[0, 0, 2 * part : 2 * part + 2] = u.astype(BF16).reshape(2, ROWS, HD)
            for half in range(2 * part, 2 * part + 2):
                remote(
                    kvbuf.at[0, 0, half], kvbuf.at[0, 2, half],
                    xss.at[0], xrs.at[half], xo,
                ).start()
                hops(1, 0, half, True)

        first(0, rotary(projected(0)))
        step3(1)
        first(1, projected(1))
        cross(0, 0, 0).start()

        def between(half, work):
            if work and half % (PIECES // 2) == PIECES // 2 - 1:
                work[half // (PIECES // 2)]()

        def turn(s, ab, work=None):
            for half in range(PIECES):
                landed(s - 1, ab, half)
                hops(s, ab, half)
                between(half, work)

        turn(2, 0)
        for half in range(PIECES):
            awaited(kvbuf.at[0, 2, half], xrs.at[half])
            hops(1, 1, half, True)
        cross(0, 2, 1).start()

        def early(s, _):
            turn(s, 0)
            turn(s - 1, 1)
            cross(s - 2, pl.ds(0, 4), 0).start()
            return 0

        lax.fori_loop(3, 6, early, 0)

        turn(6, 0)
        turn(5, 1)
        cross(4, pl.ds(0, 4), 0).start()
        turn(7, 0)
        awaited(qbuf, qrs.at[0])
        turn(6, 1, halves(lambda: group(1)))
        cross(5, pl.ds(0, 4), 0).start()
        work = halves(lambda: group(2))
        for half in range(PIECES):
            landed(HALF - 1, 0, half)
            hop((HALF - 1, half % 2), (0, 1), half, (zp, zm)[half % 2])
            between(half, work)
        cross(HALF - 1, pl.ds(0, 2), 0).start()
        turn(7, 1, halves(lambda: group(3)))
        cross(6, pl.ds(0, 4), 0).start()
        work = halves(lambda: group(4))
        for half in range(PIECES):
            landed(HALF - 1, 1, half)
            hop((HALF - 1, 2 + half % 2), (0, 3), half, (zp, zm)[half % 2])
            between(half, work)
        cross(HALF - 1, pl.ds(2, 2), 1).start()
        attend(5)
        attend_way(0)
        attend(6)
        attend(7)
        for ab in range(2):
            for half in range(PIECES):
                awaited(kvbuf.at[0, 2 * ab + 1, half], krs.at[0, ab, half])
            cross(0, 2 * ab + 1, 2 + ab).start()
        attend_way(1)
        awaited(wbuf.at[pl.ds(OS, HEADS), 0], lsem.at[1])
        for ch in range(OS, NCH):
            awaited(wbuf.at[ch, pl.ds(1, 7)], wrc.at[ch - OS])
        finish()
        awaited(wbuf.at[pl.ds(0, 2), pl.ds(0, 7)], wss.at[0])
        awaited(wbuf.at[pl.ds(0, 6), pl.ds(0, 5)], kss.at[0])
        awaited(kvbuf.at[0, 0], xss.at[0])
        awaited(kvbuf, css.at[0])

    @pl.when(c == 0)
    def _():
        awaited(wbuf.at[pl.ds(QS, 2 * HEADS), 0], lsem.at[1])
        own_x(2)
        own_x(3)
        own_x(4)
        own_x(5)
        own_x(6)
        normalize()
        give_rows()
        partner_rows()

        def near(g):
            awaited(kvbuf.at[g], crs.at[g, 0])
            attend(g)

        def near_own():
            for j, k in ((0, 0), (2, 1)):
                awaited(kvbuf.at[0, j], crs.at[0, k])
            attend_way(0)

        own_y(2)
        step1(2)
        own_y(3)
        own_y(4)
        own_y(5)
        step1(3)
        own_y(6)
        xstep1(4)
        step2(2)
        step0(7)
        step1(5)
        step2(3)
        step0(8)
        step1(6)
        xstep2(4)
        step0(9)
        step3(2)
        query(0)
        step1(7)
        step2(5)
        step0(10)
        step3(3)
        query(1)
        step1(8)
        step2(6)
        step0(11)
        xstep3(4)
        query(2)
        step1(9)
        step2(7)
        step3(5)
        query(3)
        step1(10)
        step2(8)
        step3(6)
        query(4)
        step1(11)
        step2(9)
        near_own()
        give(7)
        step2(10)
        near(1)
        give(8)
        step2(11)
        near(2)
        give(9)
        near(3)
        near(4)
        give(10)
        near(5)
        near(6)
        give(11)
        awaited(kvbuf.at[HALF - 1, pl.ds(0, 2)], crs.at[HALF - 1, 0])
        awaited(kvbuf.at[HALF - 1, pl.ds(2, 2)], crs.at[HALF - 1, 1])
        attend(7)
        for j, k in ((1, 2), (3, 3)):
            awaited(kvbuf.at[0, j], crs.at[0, k])
        attend_way(1)
        finish()
        awaited(wbuf.at[pl.ds(QS, 2 * HEADS), pl.ds(0, 7)], wss.at[0])
        awaited(wbuf.at[pl.ds(OS, HEADS), pl.ds(1, 7)], wcs.at[0])
        awaited(qout, qss.at[0])

    own = pl.ds(pl.multiple_of(c * ROWS, ROWS), ROWS)
    awaited(nrel.at[own], nss.at[0])


def local(hidden_in, attn_gain, w_query, w_keyval, w_output, post_gain):
    count, width = hidden_in.shape[1:]
    freq = 10000.0 ** (-np.arange(HD // 2) * 2.0 / HD)
    row = np.arange(2 * ROWS)[:, None] * freq
    base = np.arange(2 * NZ)[:, None] * (2 * ROWS) * freq
    tables = [np.asarray(f(a), np.float32) for a in (row, base) for f in (np.cos, np.sin)]
    vmem = pl.BlockSpec(memory_space=pltpu.VMEM)
    hbm = pl.BlockSpec(memory_space=pl.ANY)
    dma = pltpu.SemaphoreType.DMA
    operands = [
        hidden_in[0], attn_gain[None], *tables, post_gain[None],
        w_query, w_keyval, w_output,
    ]
    result = pl.pallas_call(
        ring_kernel,
        out_shape=jax.ShapeDtypeStruct((count, width), BF16),
        in_specs=[hbm] * 10,
        out_specs=vmem,
        scratch_shapes=[
            pltpu.VMEM((count, width), BF16),
            pltpu.VMEM((1, width), F32),
            pltpu.VMEM((2 * ROWS, HD // 2), F32),
            pltpu.VMEM((2 * ROWS, HD // 2), F32),
            pltpu.VMEM((2 * NZ, HD // 2), F32),
            pltpu.VMEM((2 * NZ, HD // 2), F32),
            pltpu.VMEM((1, width), F32),
            pltpu.VMEM((NCH, 8, HD, HD), BF16),
            pltpu.VMEM((HALF, 4, PIECES, ROWS, HD), BF16),
            pltpu.VMEM((2 * ROWS, 8 * HD), BF16),
            pltpu.VMEM((HEADS, ROWS, HD), BF16),
            pltpu.VMEM((HEADS, ROWS, HD), BF16),
            pltpu.VMEM((HEADS * ROWS, HD), F32),
            pltpu.VMEM((HEADS * ROWS, 128), F32),
            pltpu.VMEM((HEADS * ROWS, 128), F32),
            pltpu.VMEM((ROWS, 8 * HD), F32),
            pltpu.VMEM((2 * ROWS, HD // 2), F32),
            pltpu.VMEM((2 * ROWS, HD // 2), F32),
            pltpu.VMEM((HEADS * ROWS, 8 * ROWS), BF16),
            pltpu.VMEM((HEADS * ROWS, 128), F32),
            dma((9,)),
            dma((1,)),
            dma((1,)),
            dma((NCH, 6)),
            dma((HEADS,)),
            dma((HALF, 2, PIECES)),
            dma((1,)),
            dma((1,)),
            dma((PIECES,)),
            dma((1,)),
            dma((HALF, 4)),
            dma((1,)),
            dma((1,)),
            dma((1,)),
            dma((1,)),
        ],
        compiler_params=pltpu.CompilerParams(
            collective_id=0, has_side_effects=True, vmem_limit_bytes=40 * 1024 * 1024
        ),
    )(
        *(pltpu.with_memory_space_constraint(a, pltpu.HBM) for a in operands)
    )
    return result[None]


def solution(mesh):
    return jax.shard_map(
        local,
        mesh=mesh,
        in_specs=(
            P("dp", "seq", None), P(), P("dp", None), P("dp", None), P(None, "dp"), P(),
        ),
        out_specs=P("dp", "seq", None),
        check_vma=False,
    )
```
